32 devices in a mesh: grp: 4 (over y, x), tp: 8 (over z, core).
Axes of the slice: x: 2, y: 2, z: 4, core: 2. Of those that a mesh axis runs over, the one named last changes fastest.
Arguments:
- tokens: bfloat16 [1280, 4096], P(('grp', 'tp')), may hold values from -6 to 6
- norm_gain: float32 [4096], replicated, may hold values from 0.5 to 1.5
- spill_blocks: int32 [1], replicated, may hold values from 0 to 7, as said below
- image_gate: bfloat16 [4096, 11008], P('grp', 'tp'), may hold values from -0.09375 to 0.09375
- image_up: bfloat16 [4096, 11008], P('grp', 'tp'), may hold values from -0.09375 to 0.09375
- image_down: bfloat16 [11008, 4096], P('tp', 'grp'), may hold values from -0.0546875 to 0.0546875
- text_gate: bfloat16 [4096, 11008], P(None, 'tp'), may hold values from -0.09375 to 0.09375
- text_up: bfloat16 [4096, 11008], P(None, 'tp'), may hold values from -0.09375 to 0.09375
- text_down: bfloat16 [11008, 4096], P('tp'), may hold values from -0.0546875 to 0.0546875
Outputs:
- mixed: bfloat16 [1280, 4096], P(('grp', 'tp'))
The draws below stay inside these ranges and needn't reach their ends.
Inputs may be any that keep to these rules, and one draw needn't show every extreme that they name: `spill_blocks`: 1 distinct indices of 0 to 8 - 1, in increasing order.
All inputs are finite; a program needn't handle non-finite values.
Results may differ from the reference program's by a relative error of at most 0.0046.
Values may be sent and summed in bfloat16 or wider, within the bound.
No kernel may reach another device: no remote copies, remote signals or barrier semaphores. Data moves between devices by JAX's collectives and lax.ppermute only.
A program may use at most 256 MiB of HBM per device.

```python
import jax
import jax.numpy as jnp
from jax import lax

D = 4096
FF = 11008
TOK_DEV = 40
SPILL = 1
TOKENS = 1280
N_GRP = 4
N_TP = 8


def draw_spill_blocks(key, part):
    order = jax.random.permutation(jax.random.fold_in(key, 7), N_TP)
    return jnp.sort(order[:SPILL]).astype(jnp.int32)


def steps_of(stream_key, extent, pieces, low, top_value):
    level, own = 1.0, jax.random.fold_in(stream_key, 6)
    for position, parts in pieces:
        draws = jnp.exp(jax.random.uniform(jax.random.fold_in(own, position), (parts,), jnp.float32, low / len(pieces), top_value / len(pieces)))
        level = level * jnp.repeat(draws, extent[position] // parts).reshape([-1 if axis == position else 1 for axis in range(len(extent))])
    return level


def centred(stream_key, extent, spread, most, pieces=(), kind=jnp.bfloat16):
    factor_of = steps_of(stream_key, extent, pieces, -0.22, 0.18) if pieces else 1.0
    values = jax.random.normal(stream_key, extent, jnp.float32) * spread * factor_of
    return jnp.minimum(jnp.maximum(values, -most), most).astype(kind)


def setup_inputs(seed: int = 0) -> dict:
    arg_keys = jax.random.split(jax.random.key(seed), 10)
    tokens = centred(arg_keys[0], (TOKENS, D), 1.0, 6.0, ((0, 32),))
    norm_gain = jnp.clip(1.0 + 0.1 * jax.random.normal(arg_keys[1], (D,), jnp.float32), 0.5, 1.5)
    spill_blocks = draw_spill_blocks(jax.random.fold_in(arg_keys[9], 71), 0)
    image_gate = centred(arg_keys[3], (D, FF), D ** -0.5, 0.09375, ((0, 4), (1, 8)))
    image_up = centred(arg_keys[4], (D, FF), D ** -0.5, 0.09375, ((0, 4), (1, 8)))
    image_down = centred(arg_keys[5], (FF, D), FF ** -0.5, 0.0546875, ((0, 8), (1, 4)))
    text_gate = centred(arg_keys[6], (D, FF), D ** -0.5, 0.09375, ((1, 8),))
    text_up = centred(arg_keys[7], (D, FF), D ** -0.5, 0.09375, ((1, 8),))
    text_down = centred(arg_keys[8], (FF, D), FF ** -0.5, 0.0546875, ((0, 8),))
    return dict(tokens=tokens, norm_gain=norm_gain, spill_blocks=spill_blocks, image_gate=image_gate, image_up=image_up, image_down=image_down, text_gate=text_gate, text_up=text_up, text_down=text_down)


norm_epsilon = 1e-05

def feed_forward(inputs, w_gate, w_up, w_down):
    gate_out = jnp.dot(inputs, w_gate, preferred_element_type=jnp.float32)
    up_out = jnp.dot(inputs, w_up, preferred_element_type=jnp.float32)
    hidden = (jax.nn.silu(gate_out) * up_out).astype(jnp.bfloat16)
    return jnp.dot(hidden, w_down, preferred_element_type=jnp.float32)

def reference(tokens, norm_gain, spill_blocks, image_gate, image_up, image_down, text_gate, text_up, text_down):
    model_width = tokens.shape[1]
    tokens_wide = tokens.astype(jnp.float32)
    scale = lax.rsqrt(lax.optimization_barrier(jnp.mean(tokens_wide * tokens_wide, axis=-1, keepdims=True)) + norm_epsilon)
    normed = (tokens_wide * scale * norm_gain).astype(jnp.bfloat16)
    blocks = normed.reshape(N_GRP * N_TP, TOK_DEV, model_width)
    image_count = (N_GRP - 1) * N_TP
    text_part = blocks[image_count:]
    spill_mask = jnp.any(jnp.arange(N_TP, dtype=jnp.int32)[:, None] == spill_blocks[None, :], axis=1)
    text_ids = jnp.nonzero(jnp.logical_not(spill_mask), size=N_TP - SPILL)[0].astype(jnp.int32)
    image_rows = jnp.concatenate([blocks[:image_count], text_part[spill_blocks]], axis=0).reshape(-1, model_width)
    text_rows = text_part[text_ids].reshape(-1, model_width)
    image_out = feed_forward(image_rows, image_gate, image_up, image_down).reshape(-1, TOK_DEV, model_width)
    text_out = feed_forward(text_rows, text_gate, text_up, text_down).reshape(-1, TOK_DEV, model_width)
    text_branch = jnp.zeros((N_TP, TOK_DEV, model_width), jnp.float32)
    text_branch = text_branch.at[spill_blocks].set(image_out[image_count:]).at[text_ids].set(text_out)
    branch = jnp.concatenate([image_out[:image_count], text_branch], axis=0).reshape(-1, model_width)
    return (tokens_wide + branch).astype(jnp.bfloat16)
```

```python
import jax
import jax.numpy as jnp
from jax import lax
from jax.sharding import PartitionSpec as P

norm_epsilon = 1e-05

bf16 = jnp.bfloat16
f32 = jnp.float32


def dot32(a, b):
    return jnp.dot(a, b, preferred_element_type=f32)


def grp_swap(value, mask):
    count = lax.axis_size("grp")
    return lax.ppermute(value, "grp", [(g, g ^ mask) for g in range(count)])


def core_swap(value):
    count = lax.axis_size("tp")
    return lax.ppermute(value, "tp", [(t, t ^ 1) for t in range(count)])


def ring_send(value, step):
    count = lax.axis_size("tp")
    return lax.ppermute(value, "tp", [(t, (t + 2 * step) % count) for t in range(count)])


def text_pairs(target):
    count, groups = lax.axis_size("tp"), lax.axis_size("grp")
    base = (groups - 1) * count
    return [(base + t, base + target(t)) for t in range(count)]


def text_core_swap(value):
    return lax.ppermute(value, ("grp", "tp"), text_pairs(lambda t: t ^ 1))


def text_ring_send(value, step):
    count = lax.axis_size("tp")
    return lax.ppermute(value, ("grp", "tp"), text_pairs(lambda t: (t + 2 * step) % count))


def gather_tp(value, send, swap):
    chips = lax.axis_size("tp") // 2
    same = jnp.stack([value] + [send(value, k) for k in range(1, chips)])
    return jnp.stack([same, swap(same)])


def scatter_tp(own_core, other_core, send, swap):
    chips = own_core.shape[0]
    joined = own_core + swap(other_core.astype(bf16)).astype(f32)
    total = joined[0]
    for k in range(1, chips):
        total = total + send(joined[k].astype(bf16), chips - k).astype(f32)
    return total


def on_device(
    tokens, norm_gain, spill_blocks, image_gate, image_up, image_down, text_gate, text_up, text_down
):
    rows, width = tokens.shape
    shards = lax.axis_size("tp")
    chips = shards // 2
    groups = lax.axis_size("grp")
    g = lax.axis_index("grp")
    t = lax.axis_index("tp")
    part_width = width // groups
    spills = spill_blocks.shape[0]
    in_text = g == groups - 1
    wide = tokens.astype(f32)
    scale = lax.rsqrt(jnp.mean(wide * wide, axis=-1, keepdims=True) + norm_epsilon)
    normed = (wide * scale * norm_gain).astype(bf16)

    relative = g ^ jnp.arange(groups)
    cut = normed.reshape(rows, groups, part_width).transpose(1, 0, 2)
    cut = cut[relative]
    slots = jnp.stack([cut[0]] + [grp_swap(cut[j], j) for j in range(1, groups)])
    slots = slots[relative]

    place = (
        2 * ((t // 2 - jnp.arange(chips)) % chips)[None, :]
        + ((t % 2) ^ jnp.arange(2))[:, None]
    ).reshape(-1)
    hits = place[:, None] == spill_blocks[None, :]
    is_spill = jnp.any(hits, axis=1)
    spill_of = jnp.argmax(hits, axis=1)
    entry_of = jnp.argmax(hits, axis=0)

    def up_and_gate(chunk):
        got = gather_tp(slots[chunk[0] : chunk[-1] + 1], ring_send, core_swap)
        got = got.reshape(shards, len(chunk), rows, part_width)
        has_text = chunk[-1] == groups - 1
        image_slots = len(chunk) - int(has_text)
        parts = [got[:, :image_slots].reshape(-1, part_width)]
        if has_text:
            parts.append(got[:, -1][entry_of].reshape(-1, part_width))
        count = sum(p.shape[0] for p in parts)
        pad = -count % (32 * groups)
        if pad:
            parts.append(jnp.zeros((pad, part_width), bf16))
        inputs = jnp.concatenate(parts).reshape(groups, -1, part_width)[relative]
        n = inputs.shape[1]
        gate_in = inputs.reshape(2, 2, n, part_width).transpose(1, 0, 2, 3)
        gate_in = gate_in.reshape(2, 2 * n, part_width)
        up_in = inputs.reshape(2, 2 * n, part_width)
        gate_got = grp_swap(dot32(gate_in[1], image_gate).astype(bf16), 1)
        up_got = grp_swap(dot32(up_in[1], image_up).astype(bf16), 2)
        gate_half = dot32(gate_in[0], image_gate) + gate_got.astype(f32)
        up_half = dot32(up_in[0], image_up) + up_got.astype(f32)
        gate_last = grp_swap(gate_half[n:].astype(bf16), 2)
        up_last = grp_swap(up_half[n:].astype(bf16), 1)
        gate_out = gate_half[:n] + gate_last.astype(f32)
        up_out = up_half[:n] + up_last.astype(f32)
        hidden = (jax.nn.silu(gate_out) * up_out).astype(bf16)
        return hidden, count

    def down(chunk, hidden, count):
        half = hidden.shape[0] // 2
        first, second = hidden[:half], hidden[half:]
        first_x = grp_swap(first, 1)
        second_y = grp_swap(second, 2)
        first_y = grp_swap(jnp.concatenate([first, first_x]), 2)
        second_x = grp_swap(jnp.concatenate([second, second_y]), 1)
        every = jnp.concatenate(
            [
                first, second,
                first_x, second_x[:half],
                first_y[:half], second_y,
                first_y[half:], second_x[half:],
            ]
        ).reshape(groups, 2 * half, -1)[relative]
        out = dot32(every.reshape(groups * 2 * half, -1), image_down)
        has_text = chunk[-1] == groups - 1
        image_slots = len(chunk) - int(has_text)
        image_count = shards * image_slots * rows
        blocks = out[:image_count].reshape(shards, image_slots, rows, part_width)
        if has_text:
            spilled = out[image_count:count].reshape(spills, rows, part_width)[spill_of]
            spilled = jnp.where(is_spill[:, None, None], spilled, 0.0)
            blocks = jnp.concatenate([blocks, spilled[:, None]], axis=1)
        blocks = blocks.reshape(2, chips, len(chunk), rows, part_width)
        return scatter_tp(blocks[0], blocks[1], ring_send, core_swap).astype(bf16)

    cutoff = groups // 2
    chunks = (list(range(cutoff)), list(range(cutoff, groups)))
    hiddens = [up_and_gate(chunk) for chunk in chunks]

    text_in = gather_tp(normed, text_ring_send, text_core_swap).reshape(-1, width)
    text_hidden = (jax.nn.silu(dot32(text_in, text_gate)) * dot32(text_in, text_up)).astype(bf16)
    text_out = dot32(text_hidden, text_down).reshape(2, chips, rows, width)
    text_sum = scatter_tp(text_out[0], text_out[1], text_ring_send, text_core_swap)

    summed = jnp.concatenate([down(c, h, n) for c, (h, n) in zip(chunks, hiddens)])
    summed = summed[relative]
    columns = jnp.stack([summed[0]] + [grp_swap(summed[j], j) for j in range(1, groups)])
    image_sum = columns[relative].transpose(1, 0, 2).reshape(rows, width).astype(f32)
    own_spill = jnp.any(spill_blocks == t)
    use_text = jnp.logical_and(in_text, jnp.logical_not(own_spill))
    return (wide + jnp.where(use_text, text_sum, image_sum)).astype(bf16)


def solution(mesh):
    in_specs = (
        P(("grp", "tp"), None),
        P(),
        P(),
        P("grp", "tp"),
        P("grp", "tp"),
        P("tp", "grp"),
        P(None, "tp"),
        P(None, "tp"),
        P("tp", None),
    )
    out_specs = P(("grp", "tp"), None)
    return jax.shard_map(
        on_device, mesh=mesh, in_specs=in_specs, out_specs=out_specs, check_vma=False
    )
```

```python
import jax
import jax.numpy as jnp
from jax import lax
from jax.sharding import PartitionSpec as P

norm_epsilon = 1e-05

bf16 = jnp.bfloat16
f32 = jnp.float32


def dot32(a, b):
    return jnp.dot(a, b, preferred_element_type=f32)


def grp_swap(value, mask):
    count = lax.axis_size("grp")
    return lax.ppermute(value, "grp", [(g, g ^ mask) for g in range(count)])


def core_swap(value):
    count = lax.axis_size("tp")
    return lax.ppermute(value, "tp", [(t, t ^ 1) for t in range(count)])


def ring_send(value, step):
    count = lax.axis_size("tp")
    return lax.ppermute(value, "tp", [(t, (t + 2 * step) % count) for t in range(count)])


def gather_tp(value, send, swap):
    chips = lax.axis_size("tp") // 2
    same = jnp.stack([value] + [send(value, k) for k in range(1, chips)])
    return jnp.stack([same, swap(same)])


def scatter_tp(own_core, other_core, send, swap):
    chips = own_core.shape[0]
    joined = own_core + swap(other_core.astype(bf16)).astype(f32)
    total = joined[0]
    for k in range(1, chips):
        total = total + send(joined[k].astype(bf16), chips - k).astype(f32)
    return total


def flip_groups(parts, g):
    odd, high = (g % 2) == 1, (g // 2) == 1
    low = [jnp.where(odd, parts[j ^ 1], parts[j]) for j in range(4)]
    return [jnp.where(high, low[j ^ 2], low[j]) for j in range(4)]


def on_device(
    tokens, norm_gain, spill_blocks, image_gate, image_up, image_down, text_gate, text_up, text_down
):
    rows, width = tokens.shape
    shards = lax.axis_size("tp")
    chips = shards // 2
    groups = lax.axis_size("grp")
    g = lax.axis_index("grp")
    t = lax.axis_index("tp")
    part = width // groups
    text_gate = lax.dynamic_slice_in_dim(text_gate, g * part, part, 0)
    text_up = lax.dynamic_slice_in_dim(text_up, g * part, part, 0)
    text_down = lax.dynamic_slice_in_dim(text_down, g * part, part, 1)
    wide = tokens.astype(f32)
    scale = lax.rsqrt(jnp.mean(wide * wide, axis=-1, keepdims=True) + norm_epsilon)
    normed = (wide * scale * norm_gain).astype(bf16)

    text_slot = g ^ (groups - 1)
    cuts = flip_groups([normed[:, j * part : (j + 1) * part] for j in range(groups)], g)
    slots = [cuts[0]] + [grp_swap(cuts[j], j) for j in range(1, groups)]

    place = (
        2 * ((t // 2 - jnp.arange(chips)) % chips)[None, :]
        + ((t % 2) ^ jnp.arange(2))[:, None]
    ).reshape(-1)
    keeps_text = jnp.logical_not(jnp.any(place[:, None] == spill_blocks[None, :], axis=1))
    text_rows = jnp.broadcast_to(keeps_text[:, None], (shards, rows)).reshape(-1, 1)

    def product(inputs, first, image_w, text_w):
        index = jnp.clip(text_slot - first, 0, len(inputs) - 1)
        chosen = inputs[0]
        for j in range(1, len(inputs)):
            chosen = jnp.where(index == j, inputs[j], chosen)
        text_out = dot32(chosen, text_w)
        return [
            jnp.where(
                jnp.logical_and(text_rows, text_slot == first + j), text_out, dot32(x, image_w)
            )
            for j, x in enumerate(inputs)
        ]

    def gathered(values):
        stack = jnp.stack(values)
        got = gather_tp(stack, ring_send, core_swap).reshape(shards, len(values), rows, part)
        return [got[:, j].reshape(shards * rows, part) for j in range(len(values))]

    far = gathered(slots[3:])
    near = gathered(slots[:3])
    (gate_3,) = product(far, 3, image_gate, text_gate)
    gate_via_x = grp_swap(gate_3.astype(bf16), 1)
    (up_3,) = product(far, 3, image_up, text_up)
    up_via_y = grp_swap(up_3.astype(bf16), 2)
    gate_0, gate_1, gate_2 = product(near, 0, image_gate, text_gate)
    up_0, up_1, up_2 = product(near, 0, image_up, text_up)
    gate_x = grp_swap(gate_1.astype(bf16), 1)
    up_y = grp_swap(up_2.astype(bf16), 2)
    up_x = grp_swap((up_1 + up_via_y.astype(f32)).astype(bf16), 1)
    gate_y = grp_swap((gate_2 + gate_via_x.astype(f32)).astype(bf16), 2)
    gate_out = gate_0 + gate_x.astype(f32) + gate_y.astype(f32)
    up_out = up_0 + up_x.astype(f32) + up_y.astype(f32)
    hidden = (jax.nn.silu(gate_out) * up_out).astype(bf16)

    half = hidden.shape[0] // 2
    hidden_1 = grp_swap(hidden, 1)
    hidden_2 = grp_swap(hidden, 2)
    hidden_3 = jnp.concatenate([grp_swap(hidden_2[:half], 1), grp_swap(hidden_1[half:], 2)])

    def scattered(outs):
        blocks = jnp.stack([o.reshape(2, chips, rows, part) for o in outs], axis=2)
        return scatter_tp(blocks[0], blocks[1], ring_send, core_swap)

    summed_own = scattered(product([hidden], 0, image_down, text_down))
    summed_near = scattered(product([hidden_1, hidden_2], 1, image_down, text_down))
    summed_far = scattered(product([hidden_3], 3, image_down, text_down))
    summed = [summed_own[0], summed_near[0], summed_near[1], summed_far[0]]
    columns = [summed[0].astype(bf16)] + [
        grp_swap(summed[j].astype(bf16), j) for j in range(1, groups)
    ]
    branch = jnp.concatenate(flip_groups(columns, g), axis=1)
    return (wide + branch.astype(f32)).astype(bf16)


def solution(mesh):
    in_specs = (
        P(("grp", "tp"), None),
        P(),
        P(),
        P("grp", "tp"),
        P("grp", "tp"),
        P("tp", "grp"),
        P(None, "tp"),
        P(None, "tp"),
        P("tp", None),
    )
    out_specs = P(("grp", "tp"), None)
    return jax.shard_map(
        on_device, mesh=mesh, in_specs=in_specs, out_specs=out_specs, check_vma=False
    )
```
